32 devices in a mesh: section: 4 (over y, x), seq: 8 (over z, core).
Axes of the slice: x: 2, y: 2, z: 4, core: 2. Of those that a mesh axis runs over, the one named last changes fastest.
Arguments:
- stream: bfloat16 [4, 1024, 4096], P('section', 'seq'), may hold values from -4 to 4
- queries: bfloat16 [4, 1024, 4096], P('section', 'seq')
- span_kv: bfloat16 [4, 2, 1024, 512], P('section', None, 'seq')
- cache_kv: bfloat16 [4, 2, 1024, 512], P('section', None, 'seq'), may hold values from -6 to 6
- cache_len: int32 [8], replicated, may hold values from 48 to 80, as said below
- context_start: int32 [1], replicated, may hold values from 1 to 1024
- block_table: int32 [8, 8], replicated, may hold values from 0 to 1, as said below
Outputs:
- handed: bfloat16 [4, 1024, 4096], P('section', 'seq')
The draws below stay inside these ranges and needn't reach their ends.
Inputs may be any that keep to these rules, and one draw needn't show every extreme that they name: `cache_len`: some index holds exactly 80 live slots. `block_table`: the diagonal is 1 and every entry above it is 0.
All inputs are finite; a program needn't handle non-finite values.
Results may differ from the reference program's by a relative error of at most 0.006.
Values may be sent and summed in bfloat16 or wider, within the bound.
A program may use at most 64 MiB of HBM per device.

```python
import math
import jax
import jax.numpy as jnp
from jax import lax

HEAD_DIM = 128
HEADS = 32
KV_HEADS = 4
TOK_DEV = 128
CACHE_DEV = 128
GROUP = 8
LIVE_MAX = 80
TOKENS = 1024
CACHE = 1024
N_SECTION = 4
N_SEQ = 8


def shaped_pairs(key):
    base = jax.random.normal(jax.random.fold_in(key, 11), (N_SECTION, 2, TOKENS, KV_HEADS * HEAD_DIM), jnp.float32)
    return base


def draw_span_kv(key, part):
    return shaped_pairs(key).astype(jnp.bfloat16)


def draw_queries(key, part):
    noise = 2.0 * jax.random.normal(jax.random.fold_in(key, 12), (N_SECTION, TOKENS, HEADS * HEAD_DIM), jnp.float32)
    return noise.astype(jnp.bfloat16)


def draw_cache_len(key, part):
    counts = jax.random.randint(jax.random.fold_in(key, 21), (N_SEQ,), 3 * LIVE_MAX // 5, LIVE_MAX + 1)
    fullest = jax.random.randint(jax.random.fold_in(key, 22), (), 0, N_SEQ)
    return jnp.where(jnp.arange(N_SEQ) == fullest, LIVE_MAX, counts).astype(jnp.int32)


def draw_block_table(key, part):
    coins = jax.random.randint(jax.random.fold_in(key, 31), (N_SEQ, N_SEQ), 0, 4)
    row_ids = jnp.arange(N_SEQ)[:, None]
    col_ids = jnp.arange(N_SEQ)[None, :]
    lower = jnp.where(coins > 0, 1, 0)
    return jnp.where(col_ids < row_ids, lower, jnp.where(col_ids == row_ids, 1, 0)).astype(jnp.int32)


def level_of(key, shape, shards, smallest, high):
    gain = 1.0
    for position, blocks in shards:
        draws = jax.random.uniform(jax.random.fold_in(jax.random.fold_in(key, 6), position), (blocks,), jnp.float32, smallest / len(shards), high / len(shards))
        gain = gain * jnp.repeat(jnp.exp(draws), shape[position] // blocks).reshape((-1,) + (1,) * (len(shape) - 1 - position))
    return gain


def bell_draw(own_key, extent, width, most, split=(), held_as=jnp.bfloat16):
    array = width * jax.random.normal(own_key, extent, jnp.float32)
    if split:
        array = array * level_of(own_key, extent, split, -0.22, 0.18)
    return jnp.clip(array, -most, most).astype(held_as)


def setup_inputs(seed: int = 0) -> dict:
    streams_of = jax.random.split(jax.random.key(seed), 8)
    return {
        "stream": bell_draw(streams_of[0], (N_SECTION, TOKENS, HEADS * HEAD_DIM), 0.5, 4.0, ((0, 4), (1, 8))),
        "queries": draw_queries(jax.random.fold_in(streams_of[7], 71), 0),
        "span_kv": draw_span_kv(jax.random.fold_in(streams_of[7], 71), 0),
        "cache_kv": bell_draw(streams_of[3], (N_SECTION, 2, CACHE, KV_HEADS * HEAD_DIM), 1.0, 6.0, ((0, 4), (2, 8))),
        "cache_len": draw_cache_len(jax.random.fold_in(streams_of[7], 71), 0),
        "context_start": jax.random.randint(streams_of[5], (1,), 1, CACHE + 1).astype(jnp.int32),
        "block_table": draw_block_table(jax.random.fold_in(streams_of[7], 71), 0),
    }


def reference(stream, queries, span_kv, cache_kv, cache_len, context_start, block_table):
    score_scale = 1.0 / math.sqrt(HEAD_DIM)
    positions = jnp.arange(CACHE, dtype=jnp.int32)
    owner = positions // CACHE_DEV
    slot_index = positions % CACHE_DEV
    cache_open = (slot_index < cache_len[owner]) & (positions >= CACHE - context_start[0])
    key_tokens = jnp.arange(TOKENS, dtype=jnp.int32)
    outputs = []
    for layer in range(N_SECTION):
        all_keys = jnp.concatenate([cache_kv[layer, 0], span_kv[layer, 0]], 0).astype(jnp.float32)
        all_keys = all_keys.reshape(CACHE + TOKENS, KV_HEADS, HEAD_DIM)
        all_values = jnp.concatenate([cache_kv[layer, 1], span_kv[layer, 1]], 0).astype(jnp.float32)
        all_values = all_values.reshape(CACHE + TOKENS, KV_HEADS, HEAD_DIM)
        layer_queries = queries[layer]

        def one_block(block):
            rows = lax.dynamic_slice_in_dim(layer_queries, block * TOK_DEV, TOK_DEV, 0).astype(jnp.float32)
            rows = rows.reshape(TOK_DEV, KV_HEADS, GROUP, HEAD_DIM)
            scores = jnp.einsum('tkgd,nkd->ktgn', rows, all_keys, precision=lax.Precision.HIGHEST) * score_scale
            query_pos = block * TOK_DEV + jnp.arange(TOK_DEV, dtype=jnp.int32)
            table_row = block_table[block]
            span_open = (key_tokens[None, :] <= query_pos[:, None]) & (table_row[key_tokens // TOK_DEV][None, :] == 1)
            allowed = jnp.concatenate([jnp.broadcast_to(cache_open[None, :], (TOK_DEV, CACHE)), span_open], 1)
            wide_mask = allowed[None, :, None, :]
            row_top = lax.optimization_barrier(jnp.max(jnp.where(wide_mask, scores, -jnp.inf), -1, keepdims=True))
            weights = jnp.where(wide_mask, jnp.exp(scores - row_top), 0.0)
            row_total = lax.optimization_barrier(jnp.sum(weights, -1))
            rounded = lax.optimization_barrier(weights.astype(jnp.bfloat16)).astype(jnp.float32)
            mixed = jnp.einsum('ktgn,nkd->ktgd', rounded, all_values, precision=lax.Precision.HIGHEST)
            mixed = mixed / row_total[..., None]
            return mixed.transpose(1, 0, 2, 3).reshape(TOK_DEV, HEADS * HEAD_DIM).astype(jnp.bfloat16)
        attn = lax.map(one_block, jnp.arange(N_SEQ, dtype=jnp.int32)).reshape(TOKENS, HEADS * HEAD_DIM)
        layer_out = (stream[layer].astype(jnp.float32) + attn.astype(jnp.float32)).astype(jnp.bfloat16)
        outputs.append(layer_out)
    return jnp.roll(jnp.stack(outputs), 1, axis=0)
```

```python
import functools
import math

import jax
import jax.numpy as jnp
from jax import lax
from jax.experimental import pallas as pl
from jax.experimental.pallas import tpu as pltpu
from jax.sharding import PartitionSpec as P

HEAD_DIM = 128
LIVE_MAX = 80
TILE_HEADS = 2
BLOCK_HEADS = 4
LEVELS = 1
CHUNK_SHARDS = 8
FULL, CACHE, SPAN = 0, 1, 2
MESH = pl.DeviceIdType.MESH


def round_up(value, step):
    return -(-value // step) * step


def kernel(
    sizes, first_chip,
    len_ref, start_ref, table_ref, stream_hbm, query_hbm, span_hbm, cache_hbm,
    out_ref,
    pairs_all, query_v, stream_v, stage, cache_scores, span_scores,
    cache_bias, span_bias, top_v, acc_v,
    local_sem, bulk_sem, up_sem, side_sem, down_sem, recv_sem, hand_send, hand_recv,
):
    seq_count, section_count, kv_count, group_size, tok_rows, slot_rows = sizes
    section = lax.axis_index("section")
    me = lax.axis_index("seq")
    chip_count = seq_count // 2
    chip = me // 2
    parity = me - chip * 2
    partner = me + 1 - 2 * parity
    has_up = chip < chip_count - 1
    next_section = lax.rem(section + 1, section_count)
    prev_section = lax.rem(section + section_count - 1, section_count)
    tile_cols = TILE_HEADS * HEAD_DIM
    tiles_per = BLOCK_HEADS // TILE_HEADS
    blocks_per = group_size // BLOCK_HEADS
    pair_keys = 2 * tok_rows
    span_start = 2 * LIVE_MAX
    shard_rows = span_start + 2 * tok_rows
    first_shard = 2 * first_chip
    open_shards = seq_count - first_shard
    chunk_shards = open_shards if open_shards <= CHUNK_SHARDS else math.gcd(open_shards, CHUNK_SHARDS)
    chunk_keys = chunk_shards * LIVE_MAX
    chunk_lanes = round_up(chunk_keys, HEAD_DIM)
    chunks = open_shards // chunk_shards if open_shards else 0

    def piece(kind, head, shard):
        first, count = {
            FULL: (0, shard_rows), CACHE: (0, span_start), SPAN: (span_start, 2 * tok_rows)
        }[kind]
        return pairs_all.at[head, shard, pl.ds(first, count), :]

    def lower(source_chip, act):
        if first_chip == 0:
            act(FULL)
        elif first_chip == chip_count:
            act(SPAN)
        else:

            @pl.when(source_chip >= first_chip)
            def _():
                act(FULL)

            @pl.when(source_chip < first_chip)
            def _():
                act(SPAN)

    def upper(source_chip, act):
        if first_chip == 0:
            act(CACHE)
        elif first_chip < chip_count:

            @pl.when(source_chip >= first_chip)
            def _():
                act(CACHE)

    def local_copies(head):
        cols = pl.ds(pl.multiple_of(head * HEAD_DIM, HEAD_DIM), HEAD_DIM)
        parts = []
        for which in range(2):
            rows = pl.ds(which * LIVE_MAX, LIVE_MAX)
            parts.append((cache_hbm.at[0, which, pl.ds(0, LIVE_MAX), cols], rows))
            rows = pl.ds(span_start + which * tok_rows, tok_rows)
            parts.append((span_hbm.at[0, which, :, cols], rows))
        return [
            pltpu.make_async_copy(source, pairs_all.at[head, me, rows, :], local_sem.at[i, head])
            for i, (source, rows) in enumerate(parts)
        ]

    def remote(kind, head, shard, send, target):
        ref = piece(kind, head, shard)
        return pltpu.make_async_remote_copy(
            src_ref=ref, dst_ref=ref, send_sem=send, recv_sem=recv_sem.at[head, shard],
            device_id={"seq": target}, device_id_type=MESH,
        )

    def go_up(kind, head, shard):
        return remote(kind, head, shard, up_sem.at[head, shard], me + 2)

    def go_side(kind, head, shard):
        return remote(kind, head, shard, side_sem.at[head, shard], partner)

    def go_down(head, other):
        return remote(CACHE, head, me, down_sem.at[head, other], parity + 2 * other)

    def hand(tile):
        cols = pl.ds(pl.multiple_of(tile * tile_cols, tile_cols), tile_cols)
        return pltpu.make_async_remote_copy(
            src_ref=stage.at[:, cols], dst_ref=out_ref.at[0, :, cols],
            send_sem=hand_send.at[tile], recv_sem=hand_recv.at[tile],
            device_id={"section": next_section}, device_id_type=MESH,
        )

    for head in range(kv_count):
        for copy in local_copies(head):
            copy.start()
    query_copy = pltpu.make_async_copy(query_hbm.at[0], query_v, bulk_sem.at[0])
    stream_copy = pltpu.make_async_copy(stream_hbm.at[0], stream_v, bulk_sem.at[1])
    query_copy.start()
    stream_copy.start()

    barrier = pltpu.get_barrier_semaphore()

    def greet(device):
        pl.semaphore_signal(barrier, inc=1, device_id=device, device_id_type=MESH)

    @pl.loop(0, chip_count)
    def _(other):
        @pl.when(other != chip)
        def _():
            greet({"seq": parity + 2 * other})

    greet({"seq": partner})
    greet({"section": next_section})
    greet({"section": prev_section})

    first_visible = slot_rows * seq_count - start_ref[0]
    for chunk in range(chunks):
        key_col = lax.broadcasted_iota(jnp.int32, (1, chunk_lanes), 1)
        begin = first_shard + chunk * chunk_shards
        owner = jnp.full((1, chunk_lanes), begin, jnp.int32)
        live = jnp.full((1, chunk_lanes), len_ref[begin], jnp.int32)
        for step in range(1, chunk_shards):
            later = key_col >= step * LIVE_MAX
            owner = jnp.where(later, begin + step, owner)
            live = jnp.where(later, len_ref[begin + step], live)
        slot = key_col - (owner - begin) * LIVE_MAX
        cache_open = (slot < live) & (slot < LIVE_MAX)
        cache_open = cache_open & (owner * slot_rows + slot >= first_visible)
        lanes = pl.ds(chunk * chunk_lanes, chunk_lanes)
        cache_bias[:, lanes] = jnp.where(cache_open, 0.0, -jnp.inf).astype(jnp.float32)
    pair_col = lax.broadcasted_iota(jnp.int32, (1, pair_keys), 1)
    for pair in range(chip_count):
        hits = jnp.where(pair_col < tok_rows, table_ref[me, 2 * pair], table_ref[me, 2 * pair + 1])
        span_bias[pair, :, :] = jnp.where(hits == 1, 0.0, -jnp.inf).astype(jnp.float32)

    pl.semaphore_wait(barrier, chip_count - 1 + 3)

    def send_up(head):
        @pl.when(has_up)
        def _():
            lower(chip, lambda kind: go_up(kind, head, me).start())

    def send_rest(head):
        lower(chip, lambda kind: go_side(kind, head, me).start())

        @pl.loop(1, chip_count)
        def _(step):
            @pl.when(step <= chip)
            def _():
                upper(chip, lambda kind: go_down(head, chip - step).start())

    def relay(head):
        @pl.loop(1, chip_count)
        def _(step):
            @pl.when(step <= chip)
            def _():
                shard = me - 2 * step

                def act(kind):
                    go_up(kind, head, shard).wait_recv()

                    @pl.when(has_up)
                    def _():
                        go_up(kind, head, shard).start()

                    go_side(kind, head, shard).start()

                lower(chip - step, act)

    def from_above(head):
        @pl.loop(1, chip_count)
        def _(step):
            @pl.when(chip + step < chip_count)
            def _():
                shard = me + 2 * step

                def act(kind):
                    go_side(kind, head, shard).wait_recv()
                    go_side(kind, head, shard).start()

                upper(chip + step, act)

    def from_partner(head):
        @pl.loop(0, chip_count)
        def _(other):
            shard = partner + 2 * (other - chip)

            def act(kind):
                go_side(kind, head, shard).wait_recv()

            @pl.when(other <= chip)
            def _():
                lower(other, act)

            @pl.when(other > chip)
            def _():
                upper(other, act)

    factor = math.log2(math.e) / math.sqrt(HEAD_DIM)

    def query_key(rows, keys):
        return lax.dot_general(
            rows, keys, (((1,), (1,)), ((), ())), preferred_element_type=jnp.float32
        )

    def lane_top(scores):
        best = scores[:, :HEAD_DIM]
        for first in range(HEAD_DIM, scores.shape[1], HEAD_DIM):
            best = jnp.maximum(best, scores[:, first : first + HEAD_DIM])
        return best

    def weighted(scores, values):
        tops = jnp.concatenate([top_v[...]] * (scores.shape[1] // HEAD_DIM), axis=1)
        weights = jnp.exp2((scores - tops) * factor).astype(jnp.bfloat16)
        wide = jnp.concatenate([values, jnp.ones_like(values)], axis=1)
        return jnp.dot(weights, wide, preferred_element_type=jnp.float32)

    def cache_part(head, chunk, which):
        begin = first_shard + chunk * chunk_shards
        part = pairs_all[head, pl.ds(begin, chunk_shards), pl.ds(which * LIVE_MAX, LIVE_MAX), :]
        part = part.reshape(chunk_keys, HEAD_DIM)
        if chunk_lanes > chunk_keys:
            blank = jnp.zeros((chunk_lanes - chunk_keys, HEAD_DIM), part.dtype)
            part = jnp.concatenate([part, blank], axis=0)
        return part

    def cache_lanes(chunk):
        if chunks == 1:
            return pl.ds(0, chunk_lanes)
        return pl.ds(pl.multiple_of(chunk * chunk_lanes, HEAD_DIM), chunk_lanes)

    def span_part(head, pair, which):
        rows = pl.ds(span_start + which * tok_rows, tok_rows)
        return pairs_all[head, pl.ds(2 * pair, 2), rows, :].reshape(pair_keys, HEAD_DIM)

    def span_lanes(pair):
        return pl.ds(pl.multiple_of(pair * pair_keys, HEAD_DIM), pair_keys)

    def attend(head, block):
        def cols(index):
            first = (block * BLOCK_HEADS + index) * HEAD_DIM
            return pl.ds(pl.multiple_of(first, HEAD_DIM), HEAD_DIM)

        def rows():
            return jnp.concatenate([query_v[:, cols(i)] for i in range(BLOCK_HEADS)], axis=0)

        scores = query_key(rows(), span_part(head, chip, 0)) + span_bias[chip]
        token = lax.broadcasted_iota(jnp.int32, (tok_rows, pair_keys), 0) + parity * tok_rows
        key = lax.broadcasted_iota(jnp.int32, (tok_rows, pair_keys), 1)
        causal = jnp.concatenate([key <= token] * BLOCK_HEADS, axis=0)
        scores = jnp.where(causal, scores, -jnp.inf)
        span_scores[:, span_lanes(chip)] = scores
        top_v[...] = lane_top(scores)

        def span_scored(pair, _):
            scores = query_key(rows(), span_part(head, pair, 0)) + span_bias[pair]
            span_scores[:, span_lanes(pair)] = scores
            top_v[...] = jnp.maximum(top_v[...], lane_top(scores))
            return 0

        def cache_scored(chunk, _):
            scores = query_key(rows(), cache_part(head, chunk, 0))
            scores = scores + cache_bias[:, cache_lanes(chunk)]
            cache_scores[:, cache_lanes(chunk)] = scores
            top_v[...] = jnp.maximum(top_v[...], lane_top(scores))
            return 0

        if chunks:
            lax.fori_loop(0, chunks, cache_scored, 0)
        lax.fori_loop(0, chip, span_scored, 0)
        row_top = jnp.max(top_v[...], axis=1, keepdims=True)
        top_v[...] = jnp.broadcast_to(row_top, top_v.shape)

        def cache_mixed(chunk):
            return weighted(cache_scores[:, cache_lanes(chunk)], cache_part(head, chunk, 1))

        def span_mixed(pair):
            return weighted(span_scores[:, span_lanes(pair)], span_part(head, pair, 1))

        def cache_added(chunk, _):
            acc_v[...] += cache_mixed(chunk)
            return 0

        def span_added(pair, _):
            acc_v[...] += span_mixed(pair)
            return 0

        acc_v[...] = span_mixed(chip)
        if chunks:
            lax.fori_loop(0, chunks, cache_added, 0)
        lax.fori_loop(0, chip, span_added, 0)

    def finish(tile, part):
        for index in range(TILE_HEADS):
            first = pl.multiple_of((part * TILE_HEADS + index) * tok_rows, tok_rows)
            mixed = acc_v[pl.ds(first, tok_rows), :]
            attn = (mixed[:, :HEAD_DIM] / mixed[:, HEAD_DIM:]).astype(jnp.bfloat16)
            first = (tile * TILE_HEADS + index) * HEAD_DIM
            cols = pl.ds(pl.multiple_of(first, HEAD_DIM), HEAD_DIM)
            total = stream_v[:, cols].astype(jnp.float32) + attn.astype(jnp.float32)
            stage[:, cols] = total.astype(jnp.bfloat16)

    for head in range(kv_count):
        for copy in local_copies(head):
            copy.wait()
        if head < 2:
            send_up(head)
        send_rest(head)
    query_copy.wait()
    stream_copy.wait()

    @pl.loop(0, kv_count)
    def _(head):
        relay(head)

        @pl.when(head + 2 < kv_count)
        def _():
            send_up(head + 2)

        from_above(head)
        from_partner(head)

        @pl.loop(0, blocks_per)
        def _(inner):
            block = head * blocks_per + inner
            attend(head, block)

            @pl.loop(0, tiles_per)
            def _(part):
                tile = block * tiles_per + part
                finish(tile, part)

                @pl.when(tile > 0)
                def _():
                    hand(tile - 1).start()

    @pl.loop(0, kv_count)
    def _(head):
        @pl.loop(0, chip_count)
        def _(other):
            shard = parity + 2 * other

            @pl.when(other <= chip)
            def _():
                def act(kind):
                    go_side(kind, head, shard).wait_send()

                    @pl.when(has_up)
                    def _():
                        go_up(kind, head, shard).wait_send()

                lower(other, act)

            @pl.when(other < chip)
            def _():
                upper(chip, lambda kind: go_down(head, other).wait_send())

            @pl.when(other > chip)
            def _():
                upper(other, lambda kind: go_side(kind, head, shard).wait_send())

    tile_count = kv_count * group_size // TILE_HEADS
    hand(tile_count - 1).start()

    @pl.loop(0, tile_count)
    def _(tile):
        hand(tile).wait_recv()
        hand(tile).wait_send()


def shards(stream, queries, span_kv, cache_kv, cache_len, context_start, block_table):
    seq_count = lax.axis_size("seq")
    section_count = lax.axis_size("section")
    tok_rows, query_width = queries.shape[1:]
    key_width = span_kv.shape[3]
    kv_count = key_width // HEAD_DIM
    group_size = query_width // key_width
    slot_rows = cache_kv.shape[2]
    block_rows = BLOCK_HEADS * tok_rows
    tile_count = kv_count * group_size // TILE_HEADS
    chip_count = seq_count // 2
    sizes = (seq_count, section_count, kv_count, group_size, tok_rows, slot_rows)
    smem = pl.BlockSpec(memory_space=pltpu.SMEM)
    hbm = pl.BlockSpec(memory_space=pl.ANY)
    vmem = pl.BlockSpec(memory_space=pltpu.VMEM)
    bf16, f32 = jnp.bfloat16, jnp.float32
    dma = pltpu.SemaphoreType.DMA
    cache_width = seq_count * round_up(LIVE_MAX, HEAD_DIM)

    def call(level):
        return pl.pallas_call(
            functools.partial(kernel, sizes, level * chip_count // LEVELS),
            out_shape=pltpu.VMEM(stream.shape, bf16),
            in_specs=[smem] * 3 + [hbm] * 4,
            out_specs=vmem,
            scratch_shapes=[
                pltpu.VMEM((kv_count, seq_count, 2 * (LIVE_MAX + tok_rows), HEAD_DIM), bf16),
                pltpu.VMEM((tok_rows, query_width), bf16),
                pltpu.VMEM((tok_rows, query_width), bf16),
                pltpu.VMEM((tok_rows, query_width), bf16),
                pltpu.VMEM((block_rows, cache_width), f32),
                pltpu.VMEM((block_rows, seq_count * tok_rows), f32),
                pltpu.VMEM((1, cache_width), f32),
                pltpu.VMEM((chip_count, 1, 2 * tok_rows), f32),
                pltpu.VMEM((block_rows, HEAD_DIM), f32),
                pltpu.VMEM((block_rows, 2 * HEAD_DIM), f32),
                dma((4, kv_count)),
                dma((2,)),
                dma((kv_count, seq_count)),
                dma((kv_count, seq_count)),
                dma((kv_count, chip_count)),
                dma((kv_count, seq_count)),
                dma((tile_count,)),
                dma((tile_count,)),
            ],
            compiler_params=pltpu.CompilerParams(collective_id=level, has_side_effects=True),
        )(cache_len, context_start, block_table, stream, queries, span_kv, cache_kv)

    return call(0)


def solution(mesh):
    return jax.shard_map(
        shards,
        mesh=mesh,
        in_specs=(
            P("section", "seq", None),
            P("section", "seq", None),
            P("section", None, "seq", None),
            P("section", None, "seq", None),
            P(),
            P(),
            P(),
        ),
        out_specs=P("section", "seq", None),
        check_vma=False,
    )
```

```python
import functools
import math

import jax
import jax.numpy as jnp
from jax import lax
from jax.experimental import pallas as pl
from jax.experimental.pallas import tpu as pltpu
from jax.sharding import PartitionSpec as P

HEAD_DIM = 128
LIVE_MAX = 80
TILE_HEADS = 1
BLOCK_HEADS = 4
LEVELS = 4
FIXED_CHIPS = 4
CHUNK_SHARDS = 8
CACHE, SPAN = 0, 1
MESH = pl.DeviceIdType.MESH


def round_up(value, step):
    return -(-value // step) * step


def kernel(
    sizes, first_chip,
    len_ref, start_ref, table_ref, stream_hbm, query_hbm, span_hbm, cache_hbm,
    out_ref,
    pairs_all, query_v, stream_v, stage, cache_scores, span_scores,
    cache_bias, span_bias, top_v, acc_v,
    local_sem, bulk_sem, up_sem, side_sem, down_sem, recv_sem, hand_send, hand_recv,
):
    seq_count, section_count, kv_count, group_size, tok_rows, slot_rows = sizes
    section = lax.axis_index("section")
    me = lax.axis_index("seq")
    chip_count = seq_count // 2
    chip = me // 2
    parity = me - chip * 2
    partner = me + 1 - 2 * parity
    has_up = chip < chip_count - 1
    next_section = lax.rem(section + 1, section_count)
    prev_section = lax.rem(section + section_count - 1, section_count)
    tile_cols = TILE_HEADS * HEAD_DIM
    tiles_per = BLOCK_HEADS // TILE_HEADS
    blocks_per = group_size // BLOCK_HEADS
    pair_keys = 2 * tok_rows
    span_start = 2 * LIVE_MAX
    first_shard = 2 * first_chip
    open_shards = seq_count - first_shard
    chunk_shards = open_shards if open_shards <= CHUNK_SHARDS else math.gcd(open_shards, CHUNK_SHARDS)
    chunk_keys = chunk_shards * LIVE_MAX
    chunk_lanes = round_up(chunk_keys, HEAD_DIM)
    chunks = open_shards // chunk_shards if open_shards else 0

    def piece(kind, head, shard):
        first, count = ((0, span_start), (span_start, 2 * tok_rows))[kind]
        return pairs_all.at[head, shard, pl.ds(first, count), :]

    def upper(source_chip, act):
        if first_chip == 0:
            act(CACHE)
        elif first_chip < chip_count:

            @pl.when(source_chip >= first_chip)
            def _():
                act(CACHE)

    def lower(source_chip, act):
        upper(source_chip, act)
        act(SPAN)

    def local_copies(head):
        cols = pl.ds(pl.multiple_of(head * HEAD_DIM, HEAD_DIM), HEAD_DIM)
        parts = []
        for which in range(2):
            rows = pl.ds(which * LIVE_MAX, LIVE_MAX)
            parts.append((cache_hbm.at[0, which, pl.ds(0, LIVE_MAX), cols], rows))
            rows = pl.ds(span_start + which * tok_rows, tok_rows)
            parts.append((span_hbm.at[0, which, :, cols], rows))
        return [
            pltpu.make_async_copy(source, pairs_all.at[head, me, rows, :], local_sem.at[i, head])
            for i, (source, rows) in enumerate(parts)
        ]

    def remote(kind, head, shard, send, target):
        ref = piece(kind, head, shard)
        return pltpu.make_async_remote_copy(
            src_ref=ref, dst_ref=ref, send_sem=send, recv_sem=recv_sem.at[kind, head, shard],
            device_id={"seq": target}, device_id_type=MESH,
        )

    def go_up(kind, head, shard):
        return remote(kind, head, shard, up_sem.at[kind, head, shard], me + 2)

    def go_side(kind, head, shard):
        return remote(kind, head, shard, side_sem.at[kind, head, shard], partner)

    def go_down(head, other):
        return remote(CACHE, head, me, down_sem.at[head, other], parity + 2 * other)

    def hand(tile):
        cols = pl.ds(pl.multiple_of(tile * tile_cols, tile_cols), tile_cols)
        return pltpu.make_async_remote_copy(
            src_ref=stage.at[:, cols], dst_ref=out_ref.at[0, :, cols],
            send_sem=hand_send.at[tile], recv_sem=hand_recv.at[tile],
            device_id={"section": next_section}, device_id_type=MESH,
        )

    for head in range(kv_count):
        for copy in local_copies(head):
            copy.start()
    query_copy = pltpu.make_async_copy(query_hbm.at[0], query_v, bulk_sem.at[0])
    stream_copy = pltpu.make_async_copy(stream_hbm.at[0], stream_v, bulk_sem.at[1])

    barrier = pltpu.get_barrier_semaphore()

    def greet(device):
        pl.semaphore_signal(barrier, inc=1, device_id=device, device_id_type=MESH)

    @pl.loop(0, chip_count)
    def _(other):
        @pl.when(other != chip)
        def _():
            greet({"seq": parity + 2 * other})

    greet({"seq": partner})
    greet({"section": next_section})
    greet({"section": prev_section})

    first_visible = slot_rows * seq_count - start_ref[0]
    for chunk in range(chunks):
        key_col = lax.broadcasted_iota(jnp.int32, (1, chunk_lanes), 1)
        begin = first_shard + chunk * chunk_shards
        owner = jnp.full((1, chunk_lanes), begin, jnp.int32)
        live = jnp.full((1, chunk_lanes), len_ref[begin], jnp.int32)
        for step in range(1, chunk_shards):
            later = key_col >= step * LIVE_MAX
            owner = jnp.where(later, begin + step, owner)
            live = jnp.where(later, len_ref[begin + step], live)
        slot = key_col - (owner - begin) * LIVE_MAX
        cache_open = (slot < live) & (slot < LIVE_MAX)
        cache_open = cache_open & (owner * slot_rows + slot >= first_visible)
        lanes = pl.ds(chunk * chunk_lanes, chunk_lanes)
        cache_bias[:, lanes] = jnp.where(cache_open, 0.0, -jnp.inf).astype(jnp.float32)
    pair_col = lax.broadcasted_iota(jnp.int32, (1, pair_keys), 1)
    for pair in range(chip_count):
        hits = jnp.where(pair_col < tok_rows, table_ref[me, 2 * pair], table_ref[me, 2 * pair + 1])
        span_bias[pair, :, :] = jnp.where(hits == 1, 0.0, -jnp.inf).astype(jnp.float32)

    pl.semaphore_wait(barrier, chip_count - 1 + 3)

    def send_up(head):
        @pl.when(has_up)
        def _():
            lower(chip, lambda kind: go_up(kind, head, me).start())

    def send_side(head):
        lower(chip, lambda kind: go_side(kind, head, me).start())

    def send_down(head):
        @pl.loop(1, chip_count)
        def _(step):
            @pl.when(step <= chip)
            def _():
                upper(chip, lambda kind: go_down(head, chip - step).start())

    def relay(head, begin, end):
        @pl.loop(begin, end)
        def _(step):
            @pl.when(step <= chip)
            def _():
                shard = me - 2 * step

                def act(kind):
                    go_up(kind, head, shard).wait_recv()

                    @pl.when(has_up)
                    def _():
                        go_up(kind, head, shard).start()

                    go_side(kind, head, shard).start()

                lower(chip - step, act)

    def send_later(head):
        @pl.when((chip > 0) & (head + 1 < kv_count))
        def _():
            send_up(head + 1)

        @pl.when(head + 2 < kv_count)
        def _():
            send_down(head + 2)
            send_side(head + 2)

            @pl.when(chip == 0)
            def _():
                send_up(head + 2)

    def from_above(head):
        @pl.loop(1, chip_count)
        def _(step):
            @pl.when(chip + step < chip_count)
            def _():
                shard = me + 2 * step

                def act(kind):
                    go_side(kind, head, shard).wait_recv()
                    go_side(kind, head, shard).start()

                upper(chip + step, act)

    def from_partner(head):
        @pl.loop(0, chip_count)
        def _(other):
            shard = partner + 2 * (other - chip)

            def act(kind):
                go_side(kind, head, shard).wait_recv()

            @pl.when(other <= chip)
            def _():
                lower(other, act)

            @pl.when(other > chip)
            def _():
                upper(other, act)

    factor = math.log2(math.e) / math.sqrt(HEAD_DIM)

    def query_key(rows, keys):
        return lax.dot_general(
            rows, keys, (((1,), (1,)), ((), ())), preferred_element_type=jnp.float32
        )

    def lane_top(scores):
        best = scores[:, :HEAD_DIM]
        for first in range(HEAD_DIM, scores.shape[1], HEAD_DIM):
            best = jnp.maximum(best, scores[:, first : first + HEAD_DIM])
        return best

    def weighted(scores, values):
        tops = jnp.concatenate([top_v[...]] * (scores.shape[1] // HEAD_DIM), axis=1)
        weights = jnp.exp2((scores - tops) * factor).astype(jnp.bfloat16)
        wide = jnp.concatenate([values, jnp.ones_like(values)], axis=1)
        return jnp.dot(weights, wide, preferred_element_type=jnp.float32)

    def cache_part(head, chunk, which):
        begin = first_shard + chunk * chunk_shards
        part = pairs_all[head, pl.ds(begin, chunk_shards), pl.ds(which * LIVE_MAX, LIVE_MAX), :]
        part = part.reshape(chunk_keys, HEAD_DIM)
        if chunk_lanes > chunk_keys:
            blank = jnp.zeros((chunk_lanes - chunk_keys, HEAD_DIM), part.dtype)
            part = jnp.concatenate([part, blank], axis=0)
        return part

    def cache_lanes(chunk):
        if chunks == 1:
            return pl.ds(0, chunk_lanes)
        return pl.ds(pl.multiple_of(chunk * chunk_lanes, HEAD_DIM), chunk_lanes)

    def span_part(head, pair, which):
        rows = pl.ds(span_start + which * tok_rows, tok_rows)
        return pairs_all[head, pl.ds(2 * pair, 2), rows, :].reshape(pair_keys, HEAD_DIM)

    def span_lanes(pair):
        first = pair * pair_keys
        return pl.ds(first if isinstance(pair, int) else pl.multiple_of(first, HEAD_DIM), pair_keys)

    def attend(head, block, fixed):
        def cols(index):
            first = (block * BLOCK_HEADS + index) * HEAD_DIM
            return pl.ds(pl.multiple_of(first, HEAD_DIM), HEAD_DIM)

        def rows():
            return jnp.concatenate([query_v[:, cols(i)] for i in range(BLOCK_HEADS)], axis=0)

        scores = query_key(rows(), span_part(head, chip, 0)) + span_bias[chip]
        token = lax.broadcasted_iota(jnp.int32, (tok_rows, pair_keys), 0) + parity * tok_rows
        key = lax.broadcasted_iota(jnp.int32, (tok_rows, pair_keys), 1)
        causal = jnp.concatenate([key <= token] * BLOCK_HEADS, axis=0)
        scores = jnp.where(causal, scores, -jnp.inf)
        span_scores[:, span_lanes(chip)] = scores
        top_v[...] = lane_top(scores)

        def span_scored(pair, _):
            scores = query_key(rows(), span_part(head, pair, 0)) + span_bias[pair]
            span_scores[:, span_lanes(pair)] = scores
            top_v[...] = jnp.maximum(top_v[...], lane_top(scores))
            return 0

        def cache_scored(chunk, _):
            scores = query_key(rows(), cache_part(head, chunk, 0))
            scores = scores + cache_bias[:, cache_lanes(chunk)]
            cache_scores[:, cache_lanes(chunk)] = scores
            top_v[...] = jnp.maximum(top_v[...], lane_top(scores))
            return 0

        if chunks:
            lax.fori_loop(0, chunks, cache_scored, 0)
        if fixed is None:
            lax.fori_loop(0, chip, span_scored, 0)
        for pair in range(fixed or 0):
            span_scored(pair, 0)
        row_top = jnp.max(top_v[...], axis=1, keepdims=True)
        top_v[...] = jnp.broadcast_to(row_top, top_v.shape)

        def cache_mixed(chunk):
            return weighted(cache_scores[:, cache_lanes(chunk)], cache_part(head, chunk, 1))

        def span_mixed(pair):
            return weighted(span_scores[:, span_lanes(pair)], span_part(head, pair, 1))

        def cache_added(chunk, _):
            acc_v[...] += cache_mixed(chunk)
            return 0

        def span_added(pair, _):
            acc_v[...] += span_mixed(pair)
            return 0

        acc_v[...] = span_mixed(chip)
        if chunks:
            lax.fori_loop(0, chunks, cache_added, 0)
        if fixed is None:
            lax.fori_loop(0, chip, span_added, 0)
        for pair in range(fixed or 0):
            span_added(pair, 0)

    def finish(tile, part):
        for index in range(TILE_HEADS):
            first = pl.multiple_of((part * TILE_HEADS + index) * tok_rows, tok_rows)
            mixed = acc_v[pl.ds(first, tok_rows), :]
            attn = (mixed[:, :HEAD_DIM] / mixed[:, HEAD_DIM:]).astype(jnp.bfloat16)
            first = (tile * TILE_HEADS + index) * HEAD_DIM
            cols = pl.ds(pl.multiple_of(first, HEAD_DIM), HEAD_DIM)
            total = stream_v[:, cols].astype(jnp.float32) + attn.astype(jnp.float32)
            stage[:, cols] = total.astype(jnp.bfloat16)

    for head in range(kv_count):
        for copy in local_copies(head):
            copy.wait()
        if head < 2:
            send_down(head)
            if head == 0:
                send_up(head)
            send_side(head)
        if head == 0:
            query_copy.start()
            stream_copy.start()
    query_copy.wait()
    stream_copy.wait()

    @pl.when(chip == 0)
    def _():
        send_up(1)


    @pl.loop(0, kv_count)
    def _(head):
        @pl.when(head == 0)
        def _():
            relay(head, 1, chip_count)
            send_later(head)

        from_above(head)
        from_partner(head)

        @pl.loop(0, blocks_per)
        def _(inner):
            block = head * blocks_per + inner
            if chip_count > FIXED_CHIPS:
                attend(head, block, None)
            else:
                for fixed in range(chip_count):

                    @pl.when(chip == fixed)
                    def _():
                        attend(head, block, fixed)

            @pl.loop(0, tiles_per)
            def _(part):
                tile = block * tiles_per + part
                finish(tile, part)

                @pl.when(tile > 0)
                def _():
                    hand(tile - 1).start()

            @pl.when(head + 1 < kv_count)
            def _():
                last = inner == blocks_per - 1
                relay(head + 1, 1 + inner, jnp.where(last, chip_count, 2 + inner))

                @pl.when(last)
                def _():
                    send_later(head + 1)

    @pl.loop(0, kv_count)
    def _(head):
        @pl.loop(0, chip_count)
        def _(other):
            shard = parity + 2 * other

            @pl.when(other <= chip)
            def _():
                def act(kind):
                    go_side(kind, head, shard).wait_send()

                    @pl.when(has_up)
                    def _():
                        go_up(kind, head, shard).wait_send()

                lower(other, act)

            @pl.when(other < chip)
            def _():
                upper(chip, lambda kind: go_down(head, other).wait_send())

            @pl.when(other > chip)
            def _():
                upper(other, lambda kind: go_side(kind, head, shard).wait_send())

    tile_count = kv_count * group_size // TILE_HEADS
    hand(tile_count - 1).start()

    @pl.loop(0, tile_count)
    def _(tile):
        hand(tile).wait_recv()
        hand(tile).wait_send()


def shards(stream, queries, span_kv, cache_kv, cache_len, context_start, block_table):
    seq_count = lax.axis_size("seq")
    section_count = lax.axis_size("section")
    tok_rows, query_width = queries.shape[1:]
    key_width = span_kv.shape[3]
    kv_count = key_width // HEAD_DIM
    group_size = query_width // key_width
    slot_rows = cache_kv.shape[2]
    block_rows = BLOCK_HEADS * tok_rows
    tile_count = kv_count * group_size // TILE_HEADS
    chip_count = seq_count // 2
    sizes = (seq_count, section_count, kv_count, group_size, tok_rows, slot_rows)
    smem = pl.BlockSpec(memory_space=pltpu.SMEM)
    hbm = pl.BlockSpec(memory_space=pl.ANY)
    vmem = pl.BlockSpec(memory_space=pltpu.VMEM)
    bf16, f32 = jnp.bfloat16, jnp.float32
    dma = pltpu.SemaphoreType.DMA
    cache_width = seq_count * round_up(LIVE_MAX, HEAD_DIM)

    def call(level):
        return pl.pallas_call(
            functools.partial(kernel, sizes, level * chip_count // LEVELS),
            out_shape=pltpu.VMEM(stream.shape, bf16),
            in_specs=[smem] * 3 + [hbm] * 4,
            out_specs=vmem,
            scratch_shapes=[
                pltpu.VMEM((kv_count, seq_count, 2 * (LIVE_MAX + tok_rows), HEAD_DIM), bf16),
                pltpu.VMEM((tok_rows, query_width), bf16),
                pltpu.VMEM((tok_rows, query_width), bf16),
                pltpu.VMEM((tok_rows, query_width), bf16),
                pltpu.VMEM((block_rows, cache_width), f32),
                pltpu.VMEM((block_rows, seq_count * tok_rows), f32),
                pltpu.VMEM((1, cache_width), f32),
                pltpu.VMEM((chip_count, 1, 2 * tok_rows), f32),
                pltpu.VMEM((block_rows, HEAD_DIM), f32),
                pltpu.VMEM((block_rows, 2 * HEAD_DIM), f32),
                dma((4, kv_count)),
                dma((2,)),
                dma((2, kv_count, seq_count)),
                dma((2, kv_count, seq_count)),
                dma((kv_count, chip_count)),
                dma((2, kv_count, seq_count)),
                dma((tile_count,)),
                dma((tile_count,)),
            ],
            compiler_params=pltpu.CompilerParams(collective_id=level, has_side_effects=True),
        )(cache_len, context_start, block_table, stream, queries, span_kv, cache_kv)

    width = seq_count // LEVELS
    visible = slot_rows * seq_count - context_start[0]
    level = jnp.int32(0)
    for i in range(LEVELS):
        last_slot = (width * (i + 1) - 1) * slot_rows + LIVE_MAX - 1
        level = level + (last_slot < visible).astype(jnp.int32)
    return lax.switch(level, [functools.partial(call, i) for i in range(LEVELS + 1)])


def solution(mesh):
    return jax.shard_map(
        shards,
        mesh=mesh,
        in_specs=(
            P("section", "seq", None),
            P("section", "seq", None),
            P("section", None, "seq", None),
            P("section", None, "seq", None),
            P(),
            P(),
            P(),
        ),
        out_specs=P("section", "seq", None),
        check_vma=False,
    )
```

```python
import functools
import math

import jax
import jax.numpy as jnp
from jax import lax
from jax.experimental import pallas as pl
from jax.experimental.pallas import tpu as pltpu
from jax.sharding import PartitionSpec as P

HEAD_DIM = 128
LIVE_MAX = 80
TILE_HEADS = 1
BLOCK_HEADS = 4
LEVELS = 4
FIXED_CHIPS = 4
CHUNK_SHARDS = 8
CACHE, SPAN = 0, 1
MESH = pl.DeviceIdType.MESH


def round_up(value, step):
    return -(-value // step) * step


def kernel(
    sizes, first_chip,
    len_hbm, start_hbm, table_hbm, stream_hbm, query_hbm, span_hbm, cache_hbm,
    out_ref,
    len_ref, start_ref, table_ref,
    pairs_all, query_v, stream_v, stage, cache_scores, span_scores,
    cache_bias, span_bias, top_v, acc_v,
    table_sem, local_sem, bulk_sem, up_sem, side_sem, down_sem, recv_sem, hand_send, hand_recv,
):
    seq_count, section_count, kv_count, group_size, tok_rows, slot_rows = sizes
    section = lax.axis_index("section")
    me = lax.axis_index("seq")
    chip_count = seq_count // 2
    chip = me // 2
    parity = me - chip * 2
    partner = me + 1 - 2 * parity
    has_up = chip < chip_count - 1
    next_section = lax.rem(section + 1, section_count)
    prev_section = lax.rem(section + section_count - 1, section_count)
    tile_cols = TILE_HEADS * HEAD_DIM
    tiles_per = BLOCK_HEADS // TILE_HEADS
    blocks_per = group_size // BLOCK_HEADS
    pair_keys = 2 * tok_rows
    span_start = 2 * LIVE_MAX
    first_shard = 2 * first_chip
    open_shards = seq_count - first_shard
    chunk_shards = open_shards if open_shards <= CHUNK_SHARDS else math.gcd(open_shards, CHUNK_SHARDS)
    chunk_keys = chunk_shards * LIVE_MAX
    chunk_lanes = round_up(chunk_keys, HEAD_DIM)
    chunks = open_shards // chunk_shards if open_shards else 0

    def piece(kind, head, shard):
        first, count = ((0, span_start), (span_start, 2 * tok_rows))[kind]
        return pairs_all.at[head, shard, pl.ds(first, count), :]

    def upper(source_chip, act):
        if first_chip == 0:
            act(CACHE)
        elif first_chip < chip_count:

            @pl.when(source_chip >= first_chip)
            def _():
                act(CACHE)

    def lower(source_chip, act):
        upper(source_chip, act)
        act(SPAN)

    def local_copies(head):
        cols = pl.ds(pl.multiple_of(head * HEAD_DIM, HEAD_DIM), HEAD_DIM)
        parts = []
        for which in range(2):
            rows = pl.ds(which * LIVE_MAX, LIVE_MAX)
            parts.append((cache_hbm.at[0, which, pl.ds(0, LIVE_MAX), cols], rows))
            rows = pl.ds(span_start + which * tok_rows, tok_rows)
            parts.append((span_hbm.at[0, which, :, cols], rows))
        return [
            pltpu.make_async_copy(source, pairs_all.at[head, me, rows, :], local_sem.at[i, head])
            for i, (source, rows) in enumerate(parts)
        ]

    def remote(kind, head, shard, send, target):
        ref = piece(kind, head, shard)
        return pltpu.make_async_remote_copy(
            src_ref=ref, dst_ref=ref, send_sem=send, recv_sem=recv_sem.at[kind, head, shard],
            device_id={"seq": target}, device_id_type=MESH,
        )

    def go_up(kind, head, shard):
        return remote(kind, head, shard, up_sem.at[kind, head, shard], me + 2)

    def go_side(kind, head, shard):
        return remote(kind, head, shard, side_sem.at[kind, head, shard], partner)

    def go_down(head, other):
        return remote(CACHE, head, me, down_sem.at[head, other], parity + 2 * other)

    def hand(tile):
        cols = pl.ds(pl.multiple_of(tile * tile_cols, tile_cols), tile_cols)
        return pltpu.make_async_remote_copy(
            src_ref=stage.at[:, cols], dst_ref=out_ref.at[0, :, cols],
            send_sem=hand_send.at[tile], recv_sem=hand_recv.at[tile],
            device_id={"section": next_section}, device_id_type=MESH,
        )

    for head in range(kv_count):
        for copy in local_copies(head):
            copy.start()
    query_copy = pltpu.make_async_copy(query_hbm.at[0], query_v, bulk_sem.at[0])
    stream_copy = pltpu.make_async_copy(stream_hbm.at[0], stream_v, bulk_sem.at[1])

    tables = [
        pltpu.make_async_copy(source, target, table_sem.at[i])
        for i, (source, target) in enumerate(
            ((len_hbm, len_ref), (start_hbm, start_ref), (table_hbm, table_ref))
        )
    ]
    for copy in tables:
        copy.start()

    barrier = pltpu.get_barrier_semaphore()

    def greet(device):
        pl.semaphore_signal(barrier, inc=1, device_id=device, device_id_type=MESH)

    @pl.loop(0, chip_count)
    def _(other):
        @pl.when(other != chip)
        def _():
            greet({"seq": parity + 2 * other})

    greet({"seq": partner})
    greet({"section": next_section})
    greet({"section": prev_section})

    for copy in tables:
        copy.wait()
    first_visible = slot_rows * seq_count - start_ref[0]
    for chunk in range(chunks):
        key_col = lax.broadcasted_iota(jnp.int32, (1, chunk_lanes), 1)
        begin = first_shard + chunk * chunk_shards
        owner = jnp.full((1, chunk_lanes), begin, jnp.int32)
        live = jnp.full((1, chunk_lanes), len_ref[begin], jnp.int32)
        for step in range(1, chunk_shards):
            later = key_col >= step * LIVE_MAX
            owner = jnp.where(later, begin + step, owner)
            live = jnp.where(later, len_ref[begin + step], live)
        slot = key_col - (owner - begin) * LIVE_MAX
        cache_open = (slot < live) & (slot < LIVE_MAX)
        cache_open = cache_open & (owner * slot_rows + slot >= first_visible)
        lanes = pl.ds(chunk * chunk_lanes, chunk_lanes)
        cache_bias[:, lanes] = jnp.where(cache_open, 0.0, -jnp.inf).astype(jnp.float32)
    pair_col = lax.broadcasted_iota(jnp.int32, (1, pair_keys), 1)
    for pair in range(chip_count):
        hits = jnp.where(pair_col < tok_rows, table_ref[me, 2 * pair], table_ref[me, 2 * pair + 1])
        span_bias[pair, :, :] = jnp.where(hits == 1, 0.0, -jnp.inf).astype(jnp.float32)

    pl.semaphore_wait(barrier, chip_count - 1 + 3)

    def send_up(head):
        @pl.when(has_up)
        def _():
            lower(chip, lambda kind: go_up(kind, head, me).start())

    def send_side(head):
        lower(chip, lambda kind: go_side(kind, head, me).start())

    def send_down(head):
        @pl.loop(1, chip_count)
        def _(step):
            @pl.when(step <= chip)
            def _():
                upper(chip, lambda kind: go_down(head, chip - step).start())

    def relay(head, begin, end):
        @pl.loop(begin, end)
        def _(step):
            @pl.when(step <= chip)
            def _():
                shard = me - 2 * step

                def act(kind):
                    go_up(kind, head, shard).wait_recv()

                    @pl.when(has_up)
                    def _():
                        go_up(kind, head, shard).start()

                    go_side(kind, head, shard).start()

                lower(chip - step, act)

    def send_later(head):
        @pl.when((chip > 0) & (head + 1 < kv_count))
        def _():
            send_up(head + 1)

        @pl.when(head + 2 < kv_count)
        def _():
            send_down(head + 2)
            send_side(head + 2)

            @pl.when(chip == 0)
            def _():
                send_up(head + 2)

    def from_above(head):
        @pl.loop(1, chip_count)
        def _(step):
            @pl.when(chip + step < chip_count)
            def _():
                shard = me + 2 * step

                def act(kind):
                    go_side(kind, head, shard).wait_recv()
                    go_side(kind, head, shard).start()

                upper(chip + step, act)

    def from_partner(head):
        @pl.loop(0, chip_count)
        def _(other):
            shard = partner + 2 * (other - chip)

            def act(kind):
                go_side(kind, head, shard).wait_recv()

            @pl.when(other <= chip)
            def _():
                lower(other, act)

            @pl.when(other > chip)
            def _():
                upper(other, act)

    factor = math.log2(math.e) / math.sqrt(HEAD_DIM)

    def query_key(rows, keys):
        return lax.dot_general(
            rows, keys, (((1,), (1,)), ((), ())), preferred_element_type=jnp.float32
        )

    def lane_top(scores):
        best = scores[:, :HEAD_DIM]
        for first in range(HEAD_DIM, scores.shape[1], HEAD_DIM):
            best = jnp.maximum(best, scores[:, first : first + HEAD_DIM])
        return best

    def weighted(scores, values):
        tops = jnp.concatenate([top_v[...]] * (scores.shape[1] // HEAD_DIM), axis=1)
        weights = jnp.exp2((scores - tops) * factor).astype(jnp.bfloat16)
        wide = jnp.concatenate([values, jnp.ones_like(values)], axis=1)
        return jnp.dot(weights, wide, preferred_element_type=jnp.float32)

    def cache_part(head, chunk, which):
        begin = first_shard + chunk * chunk_shards
        part = pairs_all[head, pl.ds(begin, chunk_shards), pl.ds(which * LIVE_MAX, LIVE_MAX), :]
        part = part.reshape(chunk_keys, HEAD_DIM)
        if chunk_lanes > chunk_keys:
            blank = jnp.zeros((chunk_lanes - chunk_keys, HEAD_DIM), part.dtype)
            part = jnp.concatenate([part, blank], axis=0)
        return part

    def cache_lanes(chunk):
        if chunks == 1:
            return pl.ds(0, chunk_lanes)
        return pl.ds(pl.multiple_of(chunk * chunk_lanes, HEAD_DIM), chunk_lanes)

    def span_part(head, pair, which):
        rows = pl.ds(span_start + which * tok_rows, tok_rows)
        return pairs_all[head, pl.ds(2 * pair, 2), rows, :].reshape(pair_keys, HEAD_DIM)

    def span_lanes(pair):
        first = pair * pair_keys
        return pl.ds(first if isinstance(pair, int) else pl.multiple_of(first, HEAD_DIM), pair_keys)

    def attend(head, block, fixed):
        def cols(index):
            first = (block * BLOCK_HEADS + index) * HEAD_DIM
            return pl.ds(pl.multiple_of(first, HEAD_DIM), HEAD_DIM)

        def rows():
            return jnp.concatenate([query_v[:, cols(i)] for i in range(BLOCK_HEADS)], axis=0)

        scores = query_key(rows(), span_part(head, chip, 0)) + span_bias[chip]
        token = lax.broadcasted_iota(jnp.int32, (tok_rows, pair_keys), 0) + parity * tok_rows
        key = lax.broadcasted_iota(jnp.int32, (tok_rows, pair_keys), 1)
        causal = jnp.concatenate([key <= token] * BLOCK_HEADS, axis=0)
        scores = jnp.where(causal, scores, -jnp.inf)
        span_scores[:, span_lanes(chip)] = scores
        top_v[...] = lane_top(scores)

        def span_scored(pair, _):
            scores = query_key(rows(), span_part(head, pair, 0)) + span_bias[pair]
            span_scores[:, span_lanes(pair)] = scores
            top_v[...] = jnp.maximum(top_v[...], lane_top(scores))
            return 0

        def cache_scored(chunk, _):
            scores = query_key(rows(), cache_part(head, chunk, 0))
            scores = scores + cache_bias[:, cache_lanes(chunk)]
            cache_scores[:, cache_lanes(chunk)] = scores
            top_v[...] = jnp.maximum(top_v[...], lane_top(scores))
            return 0

        if chunks:
            lax.fori_loop(0, chunks, cache_scored, 0)
        if fixed is None:
            lax.fori_loop(0, chip, span_scored, 0)
        for pair in range(fixed or 0):
            span_scored(pair, 0)
        row_top = jnp.max(top_v[...], axis=1, keepdims=True)
        top_v[...] = jnp.broadcast_to(row_top, top_v.shape)

        def cache_mixed(chunk):
            return weighted(cache_scores[:, cache_lanes(chunk)], cache_part(head, chunk, 1))

        def span_mixed(pair):
            return weighted(span_scores[:, span_lanes(pair)], span_part(head, pair, 1))

        def cache_added(chunk, _):
            acc_v[...] += cache_mixed(chunk)
            return 0

        def span_added(pair, _):
            acc_v[...] += span_mixed(pair)
            return 0

        acc_v[...] = span_mixed(chip)
        if chunks:
            lax.fori_loop(0, chunks, cache_added, 0)
        if fixed is None:
            lax.fori_loop(0, chip, span_added, 0)
        for pair in range(fixed or 0):
            span_added(pair, 0)

    def finish(tile, part):
        for index in range(TILE_HEADS):
            first = pl.multiple_of((part * TILE_HEADS + index) * tok_rows, tok_rows)
            mixed = acc_v[pl.ds(first, tok_rows), :]
            attn = (mixed[:, :HEAD_DIM] / mixed[:, HEAD_DIM:]).astype(jnp.bfloat16)
            first = (tile * TILE_HEADS + index) * HEAD_DIM
            cols = pl.ds(pl.multiple_of(first, HEAD_DIM), HEAD_DIM)
            total = stream_v[:, cols].astype(jnp.float32) + attn.astype(jnp.float32)
            stage[:, cols] = total.astype(jnp.bfloat16)

    for head in range(kv_count):
        for copy in local_copies(head):
            copy.wait()
        if head < 2:
            send_down(head)
            if head == 0:
                send_up(head)
            send_side(head)
        if head == 0:
            query_copy.start()
            stream_copy.start()
    query_copy.wait()
    stream_copy.wait()

    @pl.when(chip == 0)
    def _():
        send_up(1)


    @pl.loop(0, kv_count)
    def _(head):
        @pl.when(head == 0)
        def _():
            relay(head, 1, chip_count)
            send_later(head)

        from_above(head)
        from_partner(head)

        @pl.loop(0, blocks_per)
        def _(inner):
            block = head * blocks_per + inner
            if chip_count > FIXED_CHIPS:
                attend(head, block, None)
            else:
                for fixed in range(chip_count):

                    @pl.when(chip == fixed)
                    def _():
                        attend(head, block, fixed)

            @pl.loop(0, tiles_per)
            def _(part):
                tile = block * tiles_per + part
                finish(tile, part)

                @pl.when(tile > 0)
                def _():
                    hand(tile - 1).start()

            @pl.when(head + 1 < kv_count)
            def _():
                last = inner == blocks_per - 1
                relay(head + 1, 1 + inner, jnp.where(last, chip_count, 2 + inner))

                @pl.when(last)
                def _():
                    send_later(head + 1)

    @pl.loop(0, kv_count)
    def _(head):
        @pl.loop(0, chip_count)
        def _(other):
            shard = parity + 2 * other

            @pl.when(other <= chip)
            def _():
                def act(kind):
                    go_side(kind, head, shard).wait_send()

                    @pl.when(has_up)
                    def _():
                        go_up(kind, head, shard).wait_send()

                lower(other, act)

            @pl.when(other < chip)
            def _():
                upper(chip, lambda kind: go_down(head, other).wait_send())

            @pl.when(other > chip)
            def _():
                upper(other, lambda kind: go_side(kind, head, shard).wait_send())

    tile_count = kv_count * group_size // TILE_HEADS
    hand(tile_count - 1).start()

    @pl.loop(0, tile_count)
    def _(tile):
        hand(tile).wait_recv()
        hand(tile).wait_send()


def shards(stream, queries, span_kv, cache_kv, cache_len, context_start, block_table):
    seq_count = lax.axis_size("seq")
    section_count = lax.axis_size("section")
    tok_rows, query_width = queries.shape[1:]
    key_width = span_kv.shape[3]
    kv_count = key_width // HEAD_DIM
    group_size = query_width // key_width
    slot_rows = cache_kv.shape[2]
    block_rows = BLOCK_HEADS * tok_rows
    tile_count = kv_count * group_size // TILE_HEADS
    chip_count = seq_count // 2
    sizes = (seq_count, section_count, kv_count, group_size, tok_rows, slot_rows)
    hbm = pl.BlockSpec(memory_space=pl.ANY)
    vmem = pl.BlockSpec(memory_space=pltpu.VMEM)
    bf16, f32 = jnp.bfloat16, jnp.float32
    dma = pltpu.SemaphoreType.DMA
    cache_width = seq_count * round_up(LIVE_MAX, HEAD_DIM)

    def in_hbm(table):
        return pltpu.with_memory_space_constraint(table, pltpu.HBM)

    def call(level):
        return pl.pallas_call(
            functools.partial(kernel, sizes, level * chip_count // LEVELS),
            out_shape=pltpu.VMEM(stream.shape, bf16),
            in_specs=[pl.BlockSpec(memory_space=pltpu.HBM)] * 3 + [hbm] * 4,
            out_specs=vmem,
            scratch_shapes=[
                pltpu.SMEM(cache_len.shape, jnp.int32),
                pltpu.SMEM(context_start.shape, jnp.int32),
                pltpu.SMEM(block_table.shape, jnp.int32),
                pltpu.VMEM((kv_count, seq_count, 2 * (LIVE_MAX + tok_rows), HEAD_DIM), bf16),
                pltpu.VMEM((tok_rows, query_width), bf16),
                pltpu.VMEM((tok_rows, query_width), bf16),
                pltpu.VMEM((tok_rows, query_width), bf16),
                pltpu.VMEM((block_rows, cache_width), f32),
                pltpu.VMEM((block_rows, seq_count * tok_rows), f32),
                pltpu.VMEM((1, cache_width), f32),
                pltpu.VMEM((chip_count, 1, 2 * tok_rows), f32),
                pltpu.VMEM((block_rows, HEAD_DIM), f32),
                pltpu.VMEM((block_rows, 2 * HEAD_DIM), f32),
                dma((3,)),
                dma((4, kv_count)),
                dma((2,)),
                dma((2, kv_count, seq_count)),
                dma((2, kv_count, seq_count)),
                dma((kv_count, chip_count)),
                dma((2, kv_count, seq_count)),
                dma((tile_count,)),
                dma((tile_count,)),
            ],
            compiler_params=pltpu.CompilerParams(collective_id=level, has_side_effects=True),
        )(in_hbm(cache_len), in_hbm(context_start), in_hbm(block_table), stream, queries, span_kv, cache_kv)

    width = seq_count // LEVELS
    visible = slot_rows * seq_count - context_start[0]
    level = jnp.int32(0)
    for i in range(LEVELS):
        last_slot = (width * (i + 1) - 1) * slot_rows + LIVE_MAX - 1
        level = level + (last_slot < visible).astype(jnp.int32)
    return lax.switch(level, [functools.partial(call, i) for i in range(LEVELS + 1)])


def solution(mesh):
    return jax.shard_map(
        shards,
        mesh=mesh,
        in_specs=(
            P("section", "seq", None),
            P("section", "seq", None),
            P("section", None, "seq", None),
            P("section", None, "seq", None),
            P(),
            P(),
            P(),
        ),
        out_specs=P("section", "seq", None),
        check_vma=False,
    )
```
